256 devices in a mesh: grp: 4 (over y, x), row: 64 (over z, core).
Axes of the slice: x: 2, y: 2, z: 32, core: 2. Of those that a mesh axis runs over, the one named last changes fastest.
The devices are a block of a 4x8x32 slice.
Arguments:
- slc: bfloat16 [2, 300, 512, 256], P(None, None, ('grp', 'row')), parts along dimension 2, may hold values from -8 to 8
- mask: int32 [25, 512, 256], P(None, ('grp', 'row')), parts along dimension 1, may hold values 0 or 1
- ref_index: int32 [4], P('grp'), parts along dimension 0, may hold values from 0 to 32767
Outputs:
- linked: float32 [2, 300, 512, 256], P(None, None, ('grp', 'row')), parts along dimension 2
The draws below stay inside these ranges and needn't reach their ends.
There are 4 independent parts, one for each index of `grp`. The reference program is written for one: setup_inputs(seed, part) draws one part's arguments, and reference() takes and returns one part's arrays. A program takes and returns all parts, laid end to end along the dimension named above; each array names one. Nothing has to cross between parts.
All inputs are finite; a program needn't handle non-finite values. No bound on the sum of `mask` on one device may be relied on, other than what follows from the above.
Results may differ from the reference program's by a relative error of at most 0.0046.
Values may be sent and summed in bfloat16 or wider, within the bound.
No kernel may reach another device: no remote copies, remote signals or barrier semaphores. Data moves between devices by JAX's collectives and lax.ppermute only.
A program may use at most 64 MiB of HBM per device.

```python
import math
import jax
import jax.numpy as jnp
from jax import lax

NDATE = 300
NC = 256
HALF = 2
ITERS = 2
OFFS = 25
NR = 128


def draw_slc(key, part):
    first, second, third = jax.random.split(key, 3)
    noise = jax.random.normal(first, (2, NDATE, NR, NC), jnp.float32)
    logamp = jax.random.uniform(second, (1, NDATE, NR, 1), jnp.float32, math.log(0.5), math.log(2.0))
    field = noise
    return jnp.clip(jnp.exp(logamp) * field, -8.0, 8.0).astype(jnp.bfloat16)


def with_ends(drawn, stream_key, smallest, high):
    longest = drawn.shape.index(max(drawn.shape))
    spots = []
    for shift in (0, 1):
        where = [jax.random.randint(jax.random.fold_in(stream_key, axis), (), 0, length) for axis, length in enumerate(drawn.shape)]
        where[longest] = (where[longest] + shift) % drawn.shape[longest]
        spots.append(tuple(where))
    return drawn.at[spots[0]].set(smallest).at[spots[1]].set(high)


def setup_inputs(seed: int = 0, part: int = 0) -> dict:
    keys = jax.random.split(jax.random.key(seed), 4)
    part_splits = jax.random.split(jax.random.fold_in(keys[3], part), 4)
    return {
        "slc": draw_slc(jax.random.fold_in(jax.random.fold_in(keys[3], part), 71), part),
        "mask": with_ends((jax.random.randint(part_splits[1], (OFFS, NR, NC), 0, 2) < 1).astype(jnp.int32), jax.random.fold_in(part_splits[1], 1), 0, 1),
        "ref_index": jax.random.randint(part_splits[2], (1,), 0, NR * NC).astype(jnp.int32),
    }


def link_pixels(extended, mask, total_rows):
    rows = extended.shape[2] - 2 * HALF
    cols = extended.shape[3]
    padded = jnp.pad(extended, ((0, 0), (0, 0), (0, 0), (HALF, HALF)))
    row_ids = jnp.arange(rows)[:, None]
    col_ids = jnp.arange(cols)[None, :]
    width = 2 * HALF + 1
    weights = []
    count = jnp.zeros((rows, cols), jnp.float32)
    for row_shift in range(-HALF, HALF + 1):
        for col_shift in range(-HALF, HALF + 1):
            offset = (row_shift + HALF) * width + col_shift + HALF
            inside = (row_ids + row_shift >= 0) & (row_ids + row_shift < total_rows)
            inside = inside & (col_ids + col_shift >= 0) & (col_ids + col_shift < cols)
            if row_shift == 0 and col_shift == 0:
                chosen = inside
            else:
                chosen = inside & (mask[offset] == 1)
            weight = chosen.astype(jnp.float32)
            weights.append(weight)
            count = count + weight
    inverse = 1.0 / count
    vector = padded[:, :, HALF:HALF + rows, HALF:HALF + cols].astype(jnp.float32)
    for step in range(ITERS):
        total_real = jnp.zeros((NDATE, rows, cols), jnp.float32)
        total_imag = jnp.zeros((NDATE, rows, cols), jnp.float32)
        for row_shift in range(-HALF, HALF + 1):
            for col_shift in range(-HALF, HALF + 1):
                offset = (row_shift + HALF) * width + col_shift + HALF
                piece = padded[:, :, HALF + row_shift:HALF + row_shift + rows, HALF + col_shift:HALF + col_shift + cols].astype(jnp.float32)
                proj_real = lax.optimization_barrier(jnp.sum(piece[0] * vector[0] + piece[1] * vector[1], axis=0)) / NDATE
                proj_imag = lax.optimization_barrier(jnp.sum(piece[0] * vector[1] - piece[1] * vector[0], axis=0)) / NDATE
                coef_real = weights[offset] * inverse * proj_real
                coef_imag = weights[offset] * inverse * proj_imag
                total_real = total_real + coef_real * piece[0] - coef_imag * piece[1]
                total_imag = total_imag + coef_real * piece[1] + coef_imag * piece[0]
        factor = lax.rsqrt(lax.optimization_barrier(jnp.mean(total_real * total_real + total_imag * total_imag, axis=0)) + 0.001)
        vector = jnp.stack([total_real * factor, total_imag * factor])
    return vector

def reference(slc, mask, ref_index):
    row_count = slc.shape[2]
    col_count = slc.shape[3]
    data = slc.astype(jnp.float32)
    power = lax.optimization_barrier(jnp.sum(data[0] * data[0] + data[1] * data[1], axis=(1, 2)))
    gains = lax.rsqrt(power / (row_count * col_count) + 0.1)
    scaled = (data * gains[:, None, None]).astype(jnp.bfloat16)
    extended = jnp.pad(scaled, ((0, 0), (0, 0), (HALF, HALF), (0, 0)))
    vector = link_pixels(extended, mask, row_count)
    target = ref_index[0].astype(jnp.int32)
    row_target = (target // col_count).astype(jnp.int32)
    col_target = (target % col_count).astype(jnp.int32)
    zero = jnp.zeros((), jnp.int32)
    picked = lax.dynamic_slice(vector, (zero, zero, row_target, col_target), (2, NDATE, 1, 1))
    real_ref = picked[0]
    imag_ref = picked[1]
    out_real = vector[0] * real_ref + vector[1] * imag_ref
    out_imag = vector[1] * real_ref - vector[0] * imag_ref
    return jnp.stack([out_real, out_imag])
```

```python
import functools

import jax
import jax.numpy as jnp
import numpy as np
from jax import lax
from jax.experimental import pallas as pl
from jax.experimental.pallas import tpu as pltpu
from jax.sharding import PartitionSpec as P

NDATE = 300
HALF = 2
ITERS = 2
WIDTH = 2 * HALF + 1
PAD = 304
REF = 384
LANES = 128
EDGE = 16
BF16 = jnp.bfloat16
F32 = jnp.float32


def swap(value, step):
    size = lax.axis_size("row")
    return lax.ppermute(value, "row", [(i, i ^ step) for i in range(size)])


def window_start(column, cols):
    return jnp.clip(column - HALF, 0, cols - WIDTH)


def scaled_by(values, gains):
    return (values.astype(F32) * gains).astype(BF16)


def reference_column(info, rows_total, near, gain):
    target_row, target_col, start = info[0], info[1], info[2]
    device = target_row // 2
    blocks = [near[(device + j + 3) % 4] for j in range(3)]
    real = jnp.concatenate([scaled_by(b[0], gain) for b in blocks], axis=0).astype(F32)
    imag = jnp.concatenate([scaled_by(b[1], gain) for b in blocks], axis=0).astype(F32)
    flags = near[(device + 4) % 4][0, 10:11, :LANES].astype(F32)
    line = lax.broadcasted_iota(jnp.int32, (48, LANES), 0)
    lane = lax.broadcasted_iota(jnp.int32, (48, LANES), 1)
    block, inner = line // 16, line % 16
    local_row, local_col = inner // WIDTH, inner % WIDTH
    a = 2 * block + local_row - target_row % 2
    b = start + local_col - target_col + HALF
    row = target_row + a - HALF
    valid = (inner < 10) & (a >= 0) & (a < WIDTH) & (b >= 0) & (b < WIDTH) & (row >= 0) & (row < rows_total)
    center = valid & (a == HALF) & (b == HALF)
    flag = jnp.sum(jnp.where(lane == a * WIDTH + b, flags, 0.0), axis=1, keepdims=True)
    valid, center = valid[:, :1], center[:, :1]
    chosen = jnp.where(center, 1.0, jnp.where(valid & (flag == 1.0), 1.0, 0.0))
    count = jnp.sum(chosen, axis=0, keepdims=True)
    weight = chosen / count
    pick = jnp.where(center, 1.0, 0.0)
    x = jnp.sum(pick * real, axis=0, keepdims=True)
    y = jnp.sum(pick * imag, axis=0, keepdims=True)
    for _ in range(ITERS):
        proj_real = jnp.sum(real * x + imag * y, axis=1, keepdims=True) / NDATE * weight
        proj_imag = jnp.sum(real * y - imag * x, axis=1, keepdims=True) / NDATE * weight
        total_real = jnp.sum(proj_real * real - proj_imag * imag, axis=0, keepdims=True)
        total_imag = jnp.sum(proj_real * imag + proj_imag * real, axis=0, keepdims=True)
        square = jnp.sum(total_real * total_real + total_imag * total_imag, axis=1, keepdims=True)
        factor = lax.rsqrt(square / NDATE + 0.001)
        x, y = total_real * factor, total_imag * factor
    both = jnp.concatenate([jnp.broadcast_to(x, (8, REF)), jnp.broadcast_to(y, (8, REF))], axis=0)
    turned = both.T
    return turned[:PAD, 0:1], turned[:PAD, 8:9]


def link_kernel(rows_total, pixels, info, power, other, straight, turned, choice, inverse, near, out, s_ref, t_ref, c_ref, d_ref, w_ref):
    total = power[...] + other[...]
    gain = lax.rsqrt(total / pixels + 0.1)
    column = jnp.broadcast_to(gain, (8, REF)).T[:PAD, 0:1]
    short = gain[:, :PAD]
    line = jnp.concatenate([short, short], axis=1)
    for t in range(2):
        for part in range(2):
            rows = pl.ds(part * PAD, PAD)
            s_ref[t, rows, :] = scaled_by(straight[t, rows, :], column)
        t_ref[t] = scaled_by(turned[t], line)
    ref_real, ref_imag = reference_column(info, rows_total, near, gain)
    c_ref[...] = jnp.zeros_like(c_ref)
    d_ref[...] = jnp.zeros_like(d_ref)
    for r in range(2):
        for t in range(2):
            k = 2 * r + t
            lanes = pl.ds((3 + r) * LANES, LANES)
            x = s_ref[t, 0:PAD, lanes]
            y = s_ref[t, PAD : 2 * PAD, lanes]
            scale = inverse[k : k + 1, :] / NDATE
            deep = pl.ds(2 * r * LANES, 6 * LANES)
            edge, main = (0, LANES) if r == 0 else (5 * LANES, 0)
            for step in range(ITERS):
                w_ref[k, 0:PAD, 0:LANES] = x
                w_ref[k, 0:PAD, LANES:] = y
                w_ref[k, PAD:, 0:LANES] = y
                w_ref[k, PAD:, LANES:] = -x
                gram = jnp.dot(
                    t_ref[t, pl.ds(r * (EDGE + LANES), 5 * LANES + EDGE), :],
                    w_ref[k],
                    preferred_element_type=F32,
                )
                real = (gram[:, :LANES] * choice[k]).astype(BF16)
                imag = (gram[:, LANES:] * choice[k]).astype(BF16)
                if r == 0:
                    pieces = ((edge, 0, EDGE), (main, EDGE, 5 * LANES))
                else:
                    pieces = ((main, 0, 5 * LANES), (edge, 5 * LANES, EDGE))
                for place, first, length in pieces:
                    c_ref[k, pl.ds(place, length), 0:LANES] = real[first : first + length]
                    c_ref[k, pl.ds(place, length), LANES:] = imag[first : first + length]
                    d_ref[k, pl.ds(place, length), 0:LANES] = -imag[first : first + length]
                    d_ref[k, pl.ds(place, length), LANES:] = real[first : first + length]
                update = jnp.dot(s_ref[t, 0:PAD, deep], c_ref[k], preferred_element_type=F32)
                update += jnp.dot(s_ref[t, PAD : 2 * PAD, deep], d_ref[k], preferred_element_type=F32)
                real, imag = update[:, :LANES], update[:, LANES:]
                square = jnp.sum(real * real + imag * imag, axis=0, keepdims=True) / NDATE
                factor = scale * lax.rsqrt(scale * scale * square + 0.001)
                real, imag = real * factor, imag * factor
                x, y = real.astype(BF16), imag.astype(BF16)
            place = pl.ds(2 * t + r, NDATE, stride=4)
            out[0, place, :] = (real * ref_real + imag * ref_imag)[:NDATE]
            out[1, place, :] = (imag * ref_real - real * ref_imag)[:NDATE]


def choices(mask, first_row, total_rows):
    rows, cols = mask.shape[1], mask.shape[2]
    row_ids = first_row + jnp.arange(rows)[:, None]
    col_ids = jnp.arange(cols)[None, :]
    weights = []
    for a in range(-HALF, HALF + 1):
        for b in range(-HALF, HALF + 1):
            inside = (row_ids + a >= 0) & (row_ids + a < total_rows)
            inside = inside & (col_ids + b >= 0) & (col_ids + b < cols)
            if (a, b) != (0, 0):
                inside = inside & (mask[(a + HALF) * WIDTH + b + HALF] == 1)
            weights.append(inside.astype(F32))
    weights = jnp.stack(weights)
    count = jnp.sum(weights, axis=0)
    tiles = weights.reshape(WIDTH, WIDTH, rows, 2, LANES)
    delta = jnp.arange(LANES)[:, None] - jnp.arange(LANES)[None, :]
    blocks = []
    for r in range(rows):
        for t in range(2):
            tile = tiles[:, :, r, t]
            main = jnp.zeros((WIDTH, LANES, LANES), F32)
            for b in range(WIDTH):
                main = jnp.where(delta[None] == b - HALF, tile[:, b][:, None, :], main)
            where = np.full((EDGE,), -1000)
            source = np.full((EDGE,), -1000)
            for e in range(6):
                for k in range(2):
                    where[2 * e + k] = LANES + k if t == 0 else k - 2
                    source[2 * e + k] = e - r
            gap = jnp.asarray(where)[:, None] - jnp.arange(LANES)[None, :]
            edge = jnp.zeros((EDGE, LANES), F32)
            for a in range(WIDTH):
                for b in range(WIDTH):
                    hit = (gap == b - HALF) & (jnp.asarray(source)[:, None] == a)
                    edge = jnp.where(hit, tile[a, b][None, :], edge)
            main = main.reshape(WIDTH * LANES, LANES)
            blocks.append(jnp.concatenate([edge, main] if r == 0 else [main, edge], axis=0))
    inverse = (1.0 / count).reshape(2 * rows, LANES)
    return jnp.stack(blocks), inverse


def layouts(previous, own, following):
    rows = jnp.concatenate([previous, own, following], axis=2)
    rows = jnp.pad(rows, ((0, 0), (0, PAD - NDATE), (0, 0), (0, 0))).reshape(2 * PAD, 6, 2 * LANES)
    straight, turned = [], []
    for t in range(2):
        main = rows[:, :, t * LANES : (t + 1) * LANES].reshape(2 * PAD, 6 * LANES)
        first = LANES if t == 0 else LANES - 2
        edge = rows[:, :, first : first + 2].reshape(2 * PAD, 12)
        wide = jnp.pad(edge, ((0, 0), (0, LANES - 12)))
        narrow = jnp.pad(edge, ((0, 0), (0, EDGE - 12))).T
        straight.append(jnp.concatenate([wide, main, wide], axis=1))
        turned.append(jnp.concatenate([narrow, main.T, narrow], axis=0))
    return jnp.stack(straight), jnp.stack(turned)


def call_link(total_rows, cols, *operands):
    vmem = pl.BlockSpec(memory_space=pltpu.VMEM)
    out = pl.pallas_call(
        functools.partial(link_kernel, total_rows, float(total_rows * cols)),
        out_shape=jax.ShapeDtypeStruct((2, NDATE * 4, LANES), F32),
        in_specs=[pl.BlockSpec(memory_space=pltpu.SMEM)] + [vmem] * 7,
        out_specs=vmem,
        scratch_shapes=[
            pltpu.VMEM((2, 2 * PAD, 8 * LANES), BF16),
            pltpu.VMEM((2, 6 * LANES + 2 * EDGE, 2 * PAD), BF16),
            pltpu.VMEM((4, 6 * LANES, 2 * LANES), BF16),
            pltpu.VMEM((4, 6 * LANES, 2 * LANES), BF16),
            pltpu.VMEM((4, 2 * PAD, 2 * LANES), BF16),
        ],
        compiler_params=pltpu.CompilerParams(vmem_limit_bytes=48 * 1024 * 1024),
        name="link",
    )(*operands)
    out = out.reshape(2, NDATE, 2, 2, LANES)
    return jnp.transpose(out, (0, 1, 3, 2, 4)).reshape(2, NDATE, 2, cols)


def per_device(slc, mask, ref_index):
    rows, cols = slc.shape[2], slc.shape[3]
    size = lax.axis_size("row")
    me = lax.axis_index("row")
    total_rows = rows * size
    squares = jnp.square(slc.astype(F32))
    power = jnp.sum(squares[0] + squares[1], axis=(1, 2))
    power = jnp.pad(power, (0, REF - NDATE))[None, :]

    target_row, target_col = ref_index[0] // cols, ref_index[0] % cols
    start = window_start(target_col, cols)
    owner = target_row // rows
    zero = jnp.zeros((), jnp.int32)
    window = lax.dynamic_slice(slc, (zero, zero, zero, start), (2, NDATE, rows, WIDTH))
    window = jnp.transpose(window, (0, 2, 3, 1)).reshape(2, rows * WIDTH, NDATE)
    flags = lax.dynamic_slice(mask, (zero, target_row % rows, target_col), (WIDTH * WIDTH, 1, 1)).reshape(1, 1, -1)
    flags = jnp.where(me == owner, flags, 0).astype(BF16)
    flags = jnp.pad(flags, ((0, 1), (0, 0), (0, NDATE - WIDTH * WIDTH)))
    window = jnp.where(jnp.abs(me - owner) <= 1, window, jnp.zeros_like(window))
    near = jnp.concatenate([window, flags, jnp.zeros((2, 16 - rows * WIDTH - 1, NDATE), BF16)], axis=1)
    near = jnp.pad(near, ((0, 0), (0, 0), (0, REF - NDATE)))

    step = size // 2
    while step >= 4:
        power, near = power + swap(power, step), near + swap(near, step)
        step //= 2
    slots = jnp.where(jnp.arange(4)[:, None, None, None] == me % 4, near[None], jnp.zeros((), BF16))
    power, slots = power + swap(power, 2), slots + swap(slots, 2)
    other, slots = swap(power, 1), slots + swap(slots, 1)

    previous = lax.ppermute(slc, "row", [(i, (i + 1) % size) for i in range(size)])
    following = lax.ppermute(slc, "row", [((i + 1) % size, i) for i in range(size)])
    straight, turned = layouts(previous, slc, following)
    choice, inverse = choices(mask, me * rows, total_rows)

    info = jnp.stack([target_row, target_col, start]).astype(jnp.int32)
    return call_link(total_rows, cols, info, power, other, straight, turned, choice, inverse, slots)


def solution(mesh):
    placed = (P(None, None, ("grp", "row"), None), P(None, ("grp", "row"), None), P("grp"))
    return jax.shard_map(
        per_device,
        mesh=mesh,
        in_specs=placed,
        out_specs=P(None, None, ("grp", "row"), None),
        check_vma=False,
    )
```

```python
import functools

import jax
import jax.numpy as jnp
import numpy as np
from jax import lax
from jax.experimental import pallas as pl
from jax.experimental.pallas import tpu as pltpu
from jax.sharding import PartitionSpec as P


NDATE = 300
HALF = 2
ITERS = 2
WIDTH = 2 * HALF + 1
PAD = 304
REF = 384
LANES = 128
DEEP = 640
SLOT = 24
HUB = 4
BASE = 2
EDGE = 16
BF16 = jnp.bfloat16
F32 = jnp.float32


def send(value, pairs):
    return lax.ppermute(value, "row", pairs)


def member(block, place):
    return (BASE + block * HUB + place) % lax.axis_size("row")


def between(source, target):
    return [(member(source, i), member(target, i)) for i in range(HUB)]


FIRST = (15, 1, 4)
THEN = (
    ((15, 12), (4, 8), (1, 2)),
    ((15, 14), (12, 10), (8, 9), (4, 6), (1, 3)),
    ((12, 13), (10, 11), (6, 7), (4, 5)),
)


def gather_order(blocks):
    return [blocks - 1] + sorted(range(1, blocks - 1), key=lambda k: -min(k, blocks - k))


def packed(power, near):
    parts = []
    for _ in range(3):
        part = lax.reduce_precision(power, exponent_bits=8, mantissa_bits=7)
        parts.append(part)
        power = power - part
    triple = jnp.concatenate(parts, axis=0).astype(BF16)[None]
    return jnp.concatenate([jnp.concatenate([near[:1, : SLOT - 3], triple], axis=1), near[1:]], axis=0)


def unpacked(message):
    return jnp.sum(message[0, SLOT - 3 :].astype(F32), axis=0, keepdims=True)


def slot_of(row):
    place = (row + 4 * HUB - BASE) % 4
    return (place % 2) * 2 + place // 2


def window_start(column, cols):
    return jnp.clip(column - HALF, 0, cols - WIDTH)


def scaled_by(values, gains):
    return (values.astype(F32) * gains).astype(BF16)


def reference_kernel(rows_total, pixels, info, near, out):
    power = jnp.sum(near[0].astype(F32)[SLOT - 3 :], axis=0, keepdims=True)
    gain = lax.rsqrt(power / pixels + 0.1)
    target_row, target_col, start = info[0], info[1], info[2]
    device = target_row // 2
    blocks = [near[slot_of(device + j - 1)].astype(F32) for j in range(3)]
    blocks = [(b * gain).astype(BF16).astype(F32) for b in blocks]
    none = jnp.zeros((2, REF), F32)
    real = jnp.concatenate([b[0:16] for b in blocks], axis=0)
    imag = jnp.concatenate([jnp.concatenate([b[10:24], none], axis=0) for b in blocks], axis=0)
    flags = near[slot_of(device)].astype(F32)[20:21, :LANES]
    line = lax.broadcasted_iota(jnp.int32, (48, LANES), 0)
    lane = lax.broadcasted_iota(jnp.int32, (48, LANES), 1)
    block, inner = line // 16, line % 16
    local_row, local_col = inner // WIDTH, inner % WIDTH
    a = 2 * block + local_row - target_row % 2
    b = start + local_col - target_col + HALF
    row = target_row + a - HALF
    valid = (inner < 10) & (a >= 0) & (a < WIDTH) & (b >= 0) & (b < WIDTH) & (row >= 0) & (row < rows_total)
    center = valid & (a == HALF) & (b == HALF)
    flag = jnp.sum(jnp.where(lane == a * WIDTH + b, flags, 0.0), axis=1, keepdims=True)
    valid, center = valid[:, :1], center[:, :1]
    chosen = jnp.where(center, 1.0, jnp.where(valid & (flag == 1.0), 1.0, 0.0))
    count = jnp.sum(chosen, axis=0, keepdims=True)
    weight = chosen / count
    pick = jnp.where(center, 1.0, 0.0)
    x = jnp.sum(pick * real, axis=0, keepdims=True)
    y = jnp.sum(pick * imag, axis=0, keepdims=True)
    for _ in range(ITERS):
        proj_real = jnp.sum(real * x + imag * y, axis=1, keepdims=True) / NDATE * weight
        proj_imag = jnp.sum(real * y - imag * x, axis=1, keepdims=True) / NDATE * weight
        total_real = jnp.sum(proj_real * real - proj_imag * imag, axis=0, keepdims=True)
        total_imag = jnp.sum(proj_real * imag + proj_imag * real, axis=0, keepdims=True)
        square = jnp.sum(total_real * total_real + total_imag * total_imag, axis=1, keepdims=True)
        factor = lax.rsqrt(square / NDATE + 0.001)
        x, y = total_real * factor, total_imag * factor
    out[...] = jnp.concatenate([power, x, y, jnp.zeros((5, REF), F32)], axis=0)


def link_kernel(pixels, straight, turned, choice, inverse, known, out, s_ref, t_ref, c_ref, d_ref, w_ref):
    gain = lax.rsqrt(known[0:1, :] / pixels + 0.1)
    columns = jnp.concatenate([gain, known[1:8, :]], axis=0).T[:PAD]
    column, ref_real, ref_imag = columns[:, 0:1], columns[:, 1:2], columns[:, 2:3]
    short = gain[:, :PAD]
    line = jnp.concatenate([short, short, jnp.zeros((1, DEEP - 2 * PAD), F32)], axis=1)
    for t in range(2):
        for part in range(2):
            rows = pl.ds(part * PAD, PAD)
            s_ref[t, rows, :] = scaled_by(straight[t, rows, :], column)
        t_ref[t] = scaled_by(turned[t], line)
    for k in range(4):
        clear = pl.ds(EDGE if k < 2 else 5 * LANES + EDGE, LANES - EDGE)
        c_ref[k, clear, :] = jnp.zeros((LANES - EDGE, 2 * LANES), BF16)
        d_ref[k, clear, :] = jnp.zeros((LANES - EDGE, 2 * LANES), BF16)
        w_ref[k, 2 * PAD :, :] = jnp.zeros((DEEP - 2 * PAD, 2 * LANES), BF16)
    for r in range(2):
        for t in range(2):
            k = 2 * r + t
            lanes = pl.ds((3 + r) * LANES, LANES)
            x = s_ref[t, 0:PAD, lanes]
            y = s_ref[t, PAD : 2 * PAD, lanes]
            scale = inverse[k : k + 1, :] / NDATE
            deep = pl.ds(2 * r * LANES, 6 * LANES)
            edge, main = (0, LANES) if r == 0 else (5 * LANES, 0)
            for _ in range(ITERS):
                w_ref[k, 0:PAD, 0:LANES] = x
                w_ref[k, 0:PAD, LANES:] = y
                w_ref[k, PAD : 2 * PAD, 0:LANES] = y
                w_ref[k, PAD : 2 * PAD, LANES:] = -x
                gram = jnp.dot(
                    t_ref[t, pl.ds(r * (EDGE + LANES), 5 * LANES + EDGE), :],
                    w_ref[k],
                    preferred_element_type=F32,
                )
                real = (gram[:, :LANES] * choice[k]).astype(BF16)
                imag = (gram[:, LANES:] * choice[k]).astype(BF16)
                if r == 0:
                    pieces = ((edge, 0, EDGE), (main, EDGE, 5 * LANES))
                else:
                    pieces = ((main, 0, 5 * LANES), (edge, 5 * LANES, EDGE))
                for place, first, length in pieces:
                    c_ref[k, pl.ds(place, length), 0:LANES] = real[first : first + length]
                    c_ref[k, pl.ds(place, length), LANES:] = imag[first : first + length]
                    d_ref[k, pl.ds(place, length), 0:LANES] = -imag[first : first + length]
                    d_ref[k, pl.ds(place, length), LANES:] = real[first : first + length]
                update = jnp.dot(s_ref[t, 0:PAD, deep], c_ref[k], preferred_element_type=F32)
                update += jnp.dot(s_ref[t, PAD : 2 * PAD, deep], d_ref[k], preferred_element_type=F32)
                real, imag = update[:, :LANES], update[:, LANES:]
                square = jnp.sum(real * real + imag * imag, axis=0, keepdims=True) / NDATE
                factor = scale * lax.rsqrt(scale * scale * square + 0.001)
                real, imag = real * factor, imag * factor
                x, y = real.astype(BF16), imag.astype(BF16)
            place = pl.ds(2 * t + r, NDATE, stride=4)
            out[0, place, :] = (real * ref_real + imag * ref_imag)[:NDATE]
            out[1, place, :] = (imag * ref_real - real * ref_imag)[:NDATE]


def choices(mask, first_row, total_rows):
    rows, cols = mask.shape[1], mask.shape[2]
    offset = jnp.arange(WIDTH * WIDTH)[:, None, None]
    row_ids = first_row + jnp.arange(rows)[None, :, None] + offset // WIDTH - HALF
    col_ids = jnp.arange(cols)[None, None, :] + offset % WIDTH - HALF
    inside = (row_ids >= 0) & (row_ids < total_rows) & (col_ids >= 0) & (col_ids < cols)
    weights = (inside & ((offset == WIDTH * HALF + HALF) | (mask == 1))).astype(F32)
    count = jnp.sum(weights, axis=0)
    tiles = weights.reshape(WIDTH, WIDTH, rows, 2, LANES)
    delta = jnp.arange(LANES)[:, None] - jnp.arange(LANES)[None, :]
    blocks = []
    for r in range(rows):
        for t in range(2):
            tile = tiles[:, :, r, t]
            main = jnp.zeros((WIDTH, LANES, LANES), F32)
            for b in range(WIDTH):
                main = jnp.where(delta[None] == b - HALF, tile[:, b][:, None, :], main)
            where = np.full((EDGE,), -1000)
            source = np.full((EDGE,), -1000)
            for e in range(6):
                for k in range(2):
                    where[2 * e + k] = LANES + k if t == 0 else k - 2
                    source[2 * e + k] = e - r
            gap = jnp.asarray(where)[:, None] - jnp.arange(LANES)[None, :]
            edge = jnp.zeros((EDGE, LANES), F32)
            for a in range(WIDTH):
                for b in range(WIDTH):
                    hit = (gap == b - HALF) & (jnp.asarray(source)[:, None] == a)
                    edge = jnp.where(hit, tile[a, b][None, :], edge)
            main = main.reshape(WIDTH * LANES, LANES)
            blocks.append(jnp.concatenate([edge, main] if r == 0 else [main, edge], axis=0))
    inverse = (1.0 / count).reshape(2 * rows, LANES)
    return jnp.stack(blocks), inverse


def layout_kernel(previous, own, following, straight, turned):
    row = lax.broadcasted_iota(jnp.int32, (2 * LANES, 2 * LANES), 0)
    lane = lax.broadcasted_iota(jnp.int32, (2 * LANES, 2 * LANES), 1)
    edge = None
    for e in range(6):
        block = (previous, own, following)[e // 2]
        left = (lane == row - LANES + 2 * e) & (row >= LANES) & (row < LANES + 2)
        right = (lane - LANES == row - LANES + 2 + 2 * e) & (row >= LANES - 2) & (row < LANES)
        pick = jnp.where(left | right, 1.0, 0.0).astype(BF16)
        part = jnp.dot(block[e % 2], pick, preferred_element_type=F32)
        edge = part if edge is None else edge + part
        for t in range(2):
            tile = block[e % 2, :, pl.ds(t * LANES, LANES)]
            straight[t, :, pl.ds((1 + e) * LANES, LANES)] = tile[: 2 * PAD]
            turned[t, pl.ds(EDGE + e * LANES, LANES), :] = tile.T
    for t in range(2):
        tile = edge[:, t * LANES : (t + 1) * LANES].astype(BF16)
        straight[t, :, 0:LANES] = tile[: 2 * PAD]
        straight[t, :, 7 * LANES :] = tile[: 2 * PAD]
        narrow = tile.T[:EDGE]
        turned[t, 0:EDGE, :] = narrow
        turned[t, EDGE + 6 * LANES :, :] = narrow


def by_row(block):
    block = jnp.pad(jnp.transpose(block, (2, 0, 1, 3)), ((0, 0), (0, 0), (0, PAD - NDATE), (0, 0)))
    block = block.reshape(2, 2 * PAD, 2 * LANES)
    return jnp.pad(block, ((0, 0), (0, DEEP - 2 * PAD), (0, 0)))


def layouts(previous, own, following):
    vmem = pl.BlockSpec(memory_space=pltpu.VMEM)
    return pl.pallas_call(
        layout_kernel,
        out_shape=(
            jax.ShapeDtypeStruct((2, 2 * PAD, 8 * LANES), BF16),
            jax.ShapeDtypeStruct((2, 6 * LANES + 2 * EDGE, DEEP), BF16),
        ),
        in_specs=[vmem] * 3,
        out_specs=(vmem, vmem),
        compiler_params=pltpu.CompilerParams(vmem_limit_bytes=16 * 1024 * 1024),
        name="layouts",
    )(by_row(previous), by_row(own), by_row(following))


def call_reference(total_rows, cols, info, near):
    vmem = pl.BlockSpec(memory_space=pltpu.VMEM)
    return pl.pallas_call(
        functools.partial(reference_kernel, total_rows, float(total_rows * cols)),
        out_shape=jax.ShapeDtypeStruct((8, REF), F32),
        in_specs=[pl.BlockSpec(memory_space=pltpu.SMEM), vmem],
        out_specs=vmem,
        compiler_params=pltpu.CompilerParams(vmem_limit_bytes=2 * 1024 * 1024),
        name="reference",
    )(info, near)


def call_link(total_rows, cols, *operands):
    vmem = pl.BlockSpec(memory_space=pltpu.VMEM)
    out = pl.pallas_call(
        functools.partial(link_kernel, float(total_rows * cols)),
        out_shape=jax.ShapeDtypeStruct((2, NDATE * 4, LANES), F32),
        in_specs=[vmem] * 5,
        out_specs=vmem,
        scratch_shapes=[
            pltpu.VMEM((2, 2 * PAD, 8 * LANES), BF16),
            pltpu.VMEM((2, 6 * LANES + 2 * EDGE, DEEP), BF16),
            pltpu.VMEM((4, 6 * LANES, 2 * LANES), BF16),
            pltpu.VMEM((4, 6 * LANES, 2 * LANES), BF16),
            pltpu.VMEM((4, DEEP, 2 * LANES), BF16),
        ],
        compiler_params=pltpu.CompilerParams(vmem_limit_bytes=16 * 1024 * 1024),
        name="link",
    )(*operands)
    out = out.reshape(2, NDATE, 2, 2, LANES)
    return jnp.transpose(out, (0, 1, 3, 2, 4)).reshape(2, NDATE, 2, cols)


def per_device(slc, mask, ref_index):
    rows, cols = slc.shape[2], slc.shape[3]
    size = lax.axis_size("row")
    me = lax.axis_index("row")
    total_rows = rows * size
    previous = send(slc, [(i, (i + 1) % size) for i in range(size)])
    following = send(slc, [((i + 1) % size, i) for i in range(size)])
    squares = jnp.square(slc.astype(F32))
    power = jnp.sum(squares[0] + squares[1], axis=(1, 2))
    power = jnp.pad(power, (0, REF - NDATE))[None, :]

    target_row, target_col = ref_index[0] // cols, ref_index[0] % cols
    start = window_start(target_col, cols)
    owner = target_row // rows
    zero = jnp.zeros((), jnp.int32)
    window = lax.dynamic_slice(slc, (zero, zero, zero, start), (2, NDATE, rows, WIDTH))
    window = jnp.transpose(window, (0, 2, 3, 1)).reshape(2 * rows * WIDTH, NDATE)
    window = jnp.where(jnp.abs(me - owner) <= 1, window, jnp.zeros_like(window))
    flags = lax.dynamic_slice(mask, (zero, target_row % rows, target_col), (WIDTH * WIDTH, 1, 1)).reshape(1, -1)
    flags = jnp.pad(jnp.where(me == owner, flags, 0).astype(BF16), ((0, 3), (0, NDATE - WIDTH * WIDTH)))
    near = jnp.pad(jnp.concatenate([window, flags], axis=0), ((0, 0), (0, REF - NDATE)))[None]

    blocks = size // HUB
    message = packed(power, near)
    arrived = []
    for k in gather_order(blocks):
        arrived.append(send(message, between(k, 0)))
    straight, turned = layouts(previous, slc, following)
    choice, inverse = choices(mask, me * rows, total_rows)
    arrived, straight, turned, choice, inverse = lax.optimization_barrier((arrived, straight, turned, choice, inverse))

    for piece in arrived:
        power, near = power + unpacked(piece), near + piece
    for step in (2, 1):
        message = packed(power, near)
        other = send(message, [(member(0, i), member(0, i ^ step)) for i in range(HUB)])
        power = power + unpacked(other)
        first = (me + HUB - BASE) // step % 2 == 0
        near = jnp.concatenate([jnp.where(first, message, other), jnp.where(first, other, message)], axis=0)
    info = jnp.stack([target_row, target_col, start]).astype(jnp.int32)
    known = call_reference(total_rows, cols, info, packed(power, near))
    known = jnp.where((me >= BASE) & (me < BASE + HUB), known, 0.0)
    received = []
    for block in FIRST:
        received.append(send(known, between(0, block)))
    for piece in received:
        known = known + piece
    for step in THEN:
        known = known + send(known, sum((between(a, b) for a, b in step), []))
    return call_link(total_rows, cols, straight, turned, choice, inverse, known)


def solution(mesh):
    placed = (P(None, None, ("grp", "row"), None), P(None, ("grp", "row"), None), P("grp"))
    return jax.shard_map(
        per_device,
        mesh=mesh,
        in_specs=placed,
        out_specs=P(None, None, ("grp", "row"), None),
        check_vma=False,
    )
```
